256 devices in a mesh: replica: 64 (over z, y, core), model: 4 (over x).
Axes of the slice: x: 4, y: 4, z: 8, core: 2. Of those that a mesh axis runs over, the one named last changes fastest.
Arguments:
- slope_query: bfloat16 [64, 1024, 1024], P('replica', None, 'model'), may hold values from -8 to 8
- slope_key: bfloat16 [64, 1024, 1024], P('replica', None, 'model'), may hold values from -8 to 8
- slope_value: bfloat16 [64, 1024, 1024], P('replica', None, 'model'), may hold values from -8 to 8
- slope_mixed: bfloat16 [64, 1024, 1024], P('replica', 'model'), may hold values from -8 to 8
- slope_norm: bfloat16 [64, 1024], P('replica'), may hold values from -16 to 16
- param_query: float32 [1024, 1024], P('replica', 'model'), may hold values from -0.5 to 0.5
- param_key: float32 [1024, 1024], P('replica', 'model'), may hold values from -0.5 to 0.5
- param_value: float32 [1024, 1024], P('replica', 'model'), may hold values from -0.5 to 0.5
- param_mixed: float32 [1024, 1024], P('model', 'replica'), may hold values from -0.5 to 0.5
- param_norm: float32 [1024], P('replica'), may hold values from 0.25 to 1.75
- state_query: float32 [1024, 1024], P('replica', 'model'), may hold values from 0.0001953125 to 0.001953125
- state_key: float32 [1024, 1024], P('replica', 'model'), may hold values from 0.0001953125 to 0.001953125
- state_value: float32 [1024, 1024], P('replica', 'model'), may hold values from 0.0001953125 to 0.001953125
- state_mixed: float32 [1024, 1024], P('model', 'replica'), may hold values from 0.0001953125 to 0.001953125
- state_norm: float32 [1024], P('replica'), may hold values from 0.05 to 0.8
Outputs:
- half_query: bfloat16 [1024, 1024], P(None, 'model')
- half_key: bfloat16 [1024, 1024], P(None, 'model')
- half_value: bfloat16 [1024, 1024], P(None, 'model')
- half_mixed: bfloat16 [1024, 1024], P('model')
- half_norm: bfloat16 [1024], replicated
- next_query: float32 [1024, 1024], P('replica', 'model')
- next_key: float32 [1024, 1024], P('replica', 'model')
- next_value: float32 [1024, 1024], P('replica', 'model')
- next_mixed: float32 [1024, 1024], P('model', 'replica')
- next_norm: float32 [1024], P('replica')
- state_new_query: float32 [1024, 1024], P('replica', 'model')
- state_new_key: float32 [1024, 1024], P('replica', 'model')
- state_new_value: float32 [1024, 1024], P('replica', 'model')
- state_new_mixed: float32 [1024, 1024], P('model', 'replica')
- state_new_norm: float32 [1024], P('replica')
The draws below stay inside these ranges and needn't reach their ends.
All inputs are finite; a program needn't handle non-finite values.
Results may differ from the reference program's by a relative error of at most 0.001.
Values may be sent and summed in bfloat16 or wider, within the bound.
No kernel may reach another device: no remote copies, remote signals or barrier semaphores. Data moves between devices by JAX's collectives and lax.ppermute only.
A program may use at most 64 MiB of HBM per device.

```python
import jax
import jax.numpy as jnp
from jax import lax

WIDTH = 1024
ATTN = 1024
REPLICAS = 64


def strengthened(array, key, source, target, shards_of, factor):
    owner, partner = [(jnp.arange(array.shape[dim]) // (array.shape[dim] // shards_of)).reshape([-1 if axis == dim else 1 for axis in range(array.ndim)]) for dim in (source, target)]
    chosen = jax.random.permutation(key, shards_of)[partner]
    strong = (owner == chosen) | (owner == (partner + shards_of // 2) % shards_of)
    return jnp.where(strong, factor * array, array)


def steps_of(own_key, shape, split, low, top_value):
    def one(position, parts):
        draws = jax.random.uniform(jax.random.fold_in(jax.random.fold_in(own_key, 6), position), (parts,), jnp.float32, low / len(split), top_value / len(split))
        return jnp.repeat(jnp.exp(draws), shape[position] // parts).reshape((-1,) + (1,) * (len(shape) - position - 1))

    factor_of = one(*split[0])
    for cut in split[1:]:
        factor_of = factor_of * one(*cut)
    return factor_of


def gaussian_with(stream_key, dims, deviation, reach, pieces, heavy, dtype=jnp.bfloat16):
    drawn = deviation * jax.random.normal(stream_key, dims, jnp.float32)
    if pieces:
        drawn = drawn * steps_of(stream_key, dims, pieces, -0.22, 0.18)
    return jnp.clip(strengthened(drawn, jax.random.fold_in(stream_key, 3), *heavy), -reach, reach).astype(dtype)


def setup_inputs(seed: int = 0) -> dict:
    streams_of = jax.random.split(jax.random.key(seed), 16)
    return {
        "slope_query": gaussian_with(streams_of[0], (REPLICAS, WIDTH, ATTN), 0.5, 8.0, ((0, 64), (2, 4)), (0, 1, 64, 4.0)),
        "slope_key": gaussian_with(streams_of[1], (REPLICAS, WIDTH, ATTN), 0.5, 8.0, ((0, 64), (2, 4)), (0, 1, 64, 4.0)),
        "slope_value": gaussian_with(streams_of[2], (REPLICAS, WIDTH, ATTN), 0.5, 8.0, ((0, 64), (2, 4)), (0, 1, 64, 4.0)),
        "slope_mixed": gaussian_with(streams_of[3], (REPLICAS, ATTN, WIDTH), 0.5, 8.0, ((0, 64), (1, 4)), (0, 2, 64, 4.0)),
        "slope_norm": gaussian_with(streams_of[4], (REPLICAS, WIDTH), 1.0, 16.0, ((0, 64),), (0, 1, 64, 4.0)),
        "param_query": gaussian_with(streams_of[5], (WIDTH, ATTN), WIDTH ** -0.5, 0.5, ((0, 64), (1, 4)), (1, 0, 64, 4.0), jnp.float32),
        "param_key": gaussian_with(streams_of[6], (WIDTH, ATTN), WIDTH ** -0.5, 0.5, ((0, 64), (1, 4)), (1, 0, 64, 4.0), jnp.float32),
        "param_value": gaussian_with(streams_of[7], (WIDTH, ATTN), WIDTH ** -0.5, 0.5, ((0, 64), (1, 4)), (1, 0, 64, 4.0), jnp.float32),
        "param_mixed": gaussian_with(streams_of[8], (ATTN, WIDTH), ATTN ** -0.5, 0.5, ((0, 4), (1, 64)), (0, 1, 64, 4.0), jnp.float32),
        "param_norm": jnp.clip(1.0 + 0.15 * jax.random.normal(streams_of[9], (WIDTH,), jnp.float32), 0.25, 1.75),
        "state_query": jnp.clip(0.0001953125 + 0.0017578125 * jax.random.uniform(streams_of[10], (WIDTH, ATTN), jnp.float32) ** steps_of(streams_of[10], (WIDTH, ATTN), ((0, 64), (1, 4)), -0.2, 0.2), 0.0001953125, 0.001953125),
        "state_key": jnp.clip(0.0001953125 + 0.0017578125 * jax.random.uniform(streams_of[11], (WIDTH, ATTN), jnp.float32) ** steps_of(streams_of[11], (WIDTH, ATTN), ((0, 64), (1, 4)), -0.2, 0.2), 0.0001953125, 0.001953125),
        "state_value": jnp.clip(0.0001953125 + 0.0017578125 * jax.random.uniform(streams_of[12], (WIDTH, ATTN), jnp.float32) ** steps_of(streams_of[12], (WIDTH, ATTN), ((0, 64), (1, 4)), -0.2, 0.2), 0.0001953125, 0.001953125),
        "state_mixed": jnp.clip(0.0001953125 + 0.0017578125 * jax.random.uniform(streams_of[13], (ATTN, WIDTH), jnp.float32) ** steps_of(streams_of[13], (ATTN, WIDTH), ((0, 4), (1, 64)), -0.2, 0.2), 0.0001953125, 0.001953125),
        "state_norm": jnp.clip(0.05 + 0.75 * jax.random.uniform(streams_of[14], (WIDTH,), jnp.float32) ** steps_of(streams_of[14], (WIDTH,), ((0, 64),), -0.2, 0.2), 0.05, 0.8),
    }


learn_rate = 0.025
hold_rate = 0.7

def reference(slope_query, slope_key, slope_value, slope_mixed, slope_norm, param_query, param_key, param_value, param_mixed, param_norm, state_query, state_key, state_value, state_mixed, state_norm):
    mean_query = lax.optimization_barrier(jnp.sum(slope_query.astype(jnp.float32), axis=0)) * REPLICAS ** (-0.5)
    mean_key = lax.optimization_barrier(jnp.sum(slope_key.astype(jnp.float32), axis=0)) * REPLICAS ** (-0.5)
    mean_value = lax.optimization_barrier(jnp.sum(slope_value.astype(jnp.float32), axis=0)) * REPLICAS ** (-0.5)
    mean_mixed = lax.optimization_barrier(jnp.sum(slope_mixed.astype(jnp.float32), axis=0)) * REPLICAS ** (-0.5)
    mean_norm = lax.optimization_barrier(jnp.sum(slope_norm.astype(jnp.float32), axis=0)) * REPLICAS ** (-0.5)
    ratio_query = jnp.sqrt(lax.optimization_barrier(jnp.sum(param_query * param_query, axis=1, keepdims=True))) * lax.rsqrt(lax.optimization_barrier(jnp.sum(mean_query * mean_query, axis=1, keepdims=True)) + 1e-06)
    mean_query = mean_query * ratio_query
    ratio_key = jnp.sqrt(lax.optimization_barrier(jnp.sum(param_key * param_key, axis=1, keepdims=True))) * lax.rsqrt(lax.optimization_barrier(jnp.sum(mean_key * mean_key, axis=1, keepdims=True)) + 1e-06)
    mean_key = mean_key * ratio_key
    ratio_value = jnp.sqrt(lax.optimization_barrier(jnp.sum(param_value * param_value, axis=1, keepdims=True))) * lax.rsqrt(lax.optimization_barrier(jnp.sum(mean_value * mean_value, axis=1, keepdims=True)) + 1e-06)
    mean_value = mean_value * ratio_value
    ratio_mixed = jnp.sqrt(lax.optimization_barrier(jnp.sum(param_mixed * param_mixed, axis=0, keepdims=True))) * lax.rsqrt(lax.optimization_barrier(jnp.sum(mean_mixed * mean_mixed, axis=0, keepdims=True)) + 1e-06)
    mean_mixed = mean_mixed * ratio_mixed
    state_new_query = hold_rate * state_query + (1.0 - hold_rate) * mean_query * mean_query
    next_query = param_query - learn_rate * mean_query * lax.rsqrt(state_new_query + 1e-06)
    state_new_key = hold_rate * state_key + (1.0 - hold_rate) * mean_key * mean_key
    next_key = param_key - learn_rate * mean_key * lax.rsqrt(state_new_key + 1e-06)
    state_new_value = hold_rate * state_value + (1.0 - hold_rate) * mean_value * mean_value
    next_value = param_value - learn_rate * mean_value * lax.rsqrt(state_new_value + 1e-06)
    state_new_mixed = hold_rate * state_mixed + (1.0 - hold_rate) * mean_mixed * mean_mixed
    next_mixed = param_mixed - learn_rate * mean_mixed * lax.rsqrt(state_new_mixed + 1e-06)
    state_new_norm = hold_rate * state_norm + (1.0 - hold_rate) * mean_norm * mean_norm
    next_norm = param_norm - learn_rate * mean_norm * lax.rsqrt(state_new_norm + 1e-06)
    half_query = next_query.astype(jnp.bfloat16)
    half_key = next_key.astype(jnp.bfloat16)
    half_value = next_value.astype(jnp.bfloat16)
    half_mixed = next_mixed.astype(jnp.bfloat16)
    half_norm = next_norm.astype(jnp.bfloat16)
    return (half_query, half_key, half_value, half_mixed, half_norm, next_query, next_key, next_value, next_mixed, next_norm, state_new_query, state_new_key, state_new_value, state_new_mixed, state_new_norm)
```

```python
import jax
import jax.numpy as jnp
from jax import lax
from jax.sharding import PartitionSpec as P

learn_rate = 0.025
hold_rate = 0.7

NZ, NY, NC, NX = 8, 4, 2, 4
F32, BF16, F16 = jnp.float32, jnp.bfloat16, jnp.float16
SCALE = 2048.0


def rid(z, y, c):
    return (z * NY + y) * NC + c


def moves(dz=0, dy=0, dc=0):
    return [
        (rid(z, y, c), rid((z + dz) % NZ, (y + dy) % NY, (c + dc) % NC))
        for z in range(NZ)
        for y in range(NY)
        for c in range(NC)
    ]


def flips(fz=0, fy=0, fc=0):
    return [
        (rid(z, y, c), rid(z ^ fz, y ^ fy, c ^ fc))
        for z in range(NZ)
        for y in range(NY)
        for c in range(NC)
    ]


ZY_GROUPS = [[rid(z, y, c) for z in range(NZ) for y in range(NY)] for c in range(NC)]
Z_GROUPS = [[rid(z, y, c) for z in range(NZ)] for y in range(NY) for c in range(NC)]
Y_GROUPS = [[rid(z, y, c) for y in range(NY)] for z in range(NZ) for c in range(NC)]
BUTTERFLY = [(0, 0, 1), (0, 1, 0), (0, 2, 0), (1, 0, 0), (2, 0, 0), (4, 0, 0)]


def exchange(value, groups):
    return lax.all_to_all(value, "replica", 0, 0, tiled=True, axis_index_groups=groups)


def from_core(value):
    return lax.ppermute(value, "replica", moves(dc=1))


def over_model(value):
    others = [
        lax.ppermute(value, "model", [(i, (i + d) % NX) for i in range(NX)])
        for d in range(1, NX)
    ]
    return (value + others[1]) + (others[0] + others[2])


def norm_path(slope, param, state, me):
    width = slope.shape[-1]
    mine = jnp.stack([param, state])
    own = lax.dynamic_update_slice(
        jnp.zeros((2, width), F32), mine, (0, me * param.shape[0])
    )
    both = jnp.concatenate([slope.astype(F32).reshape(1, width), own])
    for step in BUTTERFLY:
        both = both + lax.ppermute(both, "replica", flips(*step))
    mean = both[0] * NC**-0.5 * (NZ * NY) ** -0.5
    new = hold_rate * both[2] + (1.0 - hold_rate) * mean * mean
    nxt = both[1] - learn_rate * mean * lax.rsqrt(new + 1e-06)
    take = lambda v: lax.dynamic_slice(v, (me * param.shape[0],), param.shape)
    return nxt.astype(BF16), take(nxt), take(new)


def local(sq, sk, sv, sm, sn, pq, pk, pv, pm, pn, tq, tk, tv, tm, tn):
    me = lax.axis_index("replica")
    core = me % NC
    slopes = [sq[0], sk[0], sv[0], sm[0].T]
    params = [pq, pk, pv, pm.T]
    states = [tq, tk, tv, tm.T]
    rows, cols = pq.shape
    half_norm, next_norm, new_norm = norm_path(sn, pn, tn, me)

    cut = [s.reshape(NZ * NY, NC, rows, cols) for s in slopes]
    pick = lambda b, which: lax.dynamic_index_in_dim(b, which, 1, keepdims=False)
    sent = [from_core(pick(b, 1 - core)) for b in cut]
    part = jnp.stack(
        [
            ((pick(b, core).astype(F32) + r.astype(F32)) * SCALE).astype(F16)
            for b, r in zip(cut, sent)
        ],
        axis=1,
    )
    parts = exchange(part, ZY_GROUPS)
    parts, half_norm, next_norm, new_norm = lax.optimization_barrier(
        (parts, half_norm, next_norm, new_norm)
    )
    total = jnp.sum(parts.astype(F32), axis=0)
    mean = total * (SCALE**-1 * (NZ * NY * NC) ** -0.5)

    param = jnp.stack(params)
    state = jnp.stack(states)
    own = over_model(jnp.sum(param * param, axis=2))
    size = over_model(jnp.sum(mean * mean, axis=2))
    mean = mean * (jnp.sqrt(own) * lax.rsqrt(size + 1e-06))[:, :, None]
    new = hold_rate * state + (1.0 - hold_rate) * mean * mean
    nxt = param - learn_rate * mean * lax.rsqrt(new + 1e-06)

    half = nxt.astype(BF16)
    half = exchange(jnp.broadcast_to(half, (NZ, *half.shape)), Z_GROUPS)
    half = exchange(jnp.broadcast_to(half, (NY, *half.shape)), Y_GROUPS)
    other = from_core(half)
    first = core == 0
    both = jnp.stack([jnp.where(first, half, other), jnp.where(first, other, half)])
    whole = [
        jnp.moveaxis(both[:, :, :, k], 0, 2).swapaxes(0, 1).reshape(-1, cols)
        for k in range(4)
    ]
    return (
        whole[0],
        whole[1],
        whole[2],
        whole[3].T,
        half_norm,
        nxt[0],
        nxt[1],
        nxt[2],
        nxt[3].T,
        next_norm,
        new[0],
        new[1],
        new[2],
        new[3].T,
        new_norm,
    )


def solution(mesh):
    matrix = P("replica", "model")
    turned = P("model", "replica")
    vector = P("replica")
    slope = P("replica", None, "model")
    mine = (matrix, matrix, matrix, turned, vector)
    return jax.shard_map(
        local,
        mesh=mesh,
        in_specs=(slope, slope, slope, P("replica", "model", None), P("replica", None), *mine, *mine),
        out_specs=(P(None, "model"), P(None, "model"), P(None, "model"), P("model", None), P(), *mine, *mine),
        check_vma=False,
    )
```

```python
import jax
import jax.numpy as jnp
from jax import lax
from jax.experimental import pallas as pl
from jax.experimental.pallas import tpu as pltpu
from jax.sharding import PartitionSpec as P

learn_rate = 0.025
hold_rate = 0.7

NZ, NY, NC, NX = 8, 4, 2, 4
F32, BF16, F16 = jnp.float32, jnp.bfloat16, jnp.float16
HBM = pl.BlockSpec(memory_space=pltpu.MemorySpace.HBM)
VMEM = pl.BlockSpec(memory_space=pltpu.MemorySpace.VMEM)


def rid(z, y, c):
    return (z * NY + y) * NC + c


PLACES = [(z, y, c) for z in range(NZ) for y in range(NY) for c in range(NC)]
Z_GROUPS = [[rid(z, y, c) for z in range(NZ)] for y in range(NY) for c in range(NC)]


def along_y(value, d):
    moves = [(rid(z, y, c), rid(z, (y + d) % NY, c)) for z, y, c in PLACES]
    return lax.ppermute(value, "replica", moves)


def from_core(value):
    moves = [(rid(z, y, c), rid(z, y, 1 - c)) for z, y, c in PLACES]
    return lax.ppermute(value, "replica", moves)


def across_z(value):
    return lax.all_to_all(value, "replica", 0, 0, tiled=True, axis_index_groups=Z_GROUPS)


def over_model(value):
    for flip in (1, 3):
        value = value + lax.ppermute(value, "model", [(i, i ^ flip) for i in range(NX)])
    return value


def tied(*values):
    return lax.optimization_barrier(values)


def place():
    me = lax.axis_index("replica")
    return lax.rem(lax.div(me, NC), NY), lax.rem(me, NC)


def pack(plain, turned):
    blocks = plain[0].shape
    width, height = turned.shape
    shape = (NZ, len(plain) + 1, *blocks[3:])

    def kernel(*refs):
        count = len(plain) + 1
        ins, outs, held, across, sems = (
            refs[:count],
            refs[count : -count - 2],
            refs[-count - 2 : -2],
            refs[-2],
            refs[-1],
        )
        copies = [
            pltpu.make_async_copy(ins[i], across if i == count - 1 else held[i], sems.at[i])
            for i in range(count)
        ]
        for i in (count - 1, *range(count - 1)):
            copies[i].start()
        y, core = place()
        for i in (count - 1, *range(count - 1)):
            copies[i].wait()
            if i == count - 1:
                flipped = across[...].T.reshape(blocks)
                held[i][...] = flipped
            for d in range(NY):
                at = lax.rem(y + d, NY)
                outs[d][:, i] = held[i][:, at, 1 - core]
                outs[NY + d][:, i] = held[i][:, at, core]

    out = pl.pallas_call(
        kernel,
        out_shape=[jax.ShapeDtypeStruct(shape, BF16)] * (2 * NY),
        in_specs=[HBM] * (len(plain) + 1),
        out_specs=[VMEM] * (2 * NY),
        scratch_shapes=[pltpu.VMEM(blocks, BF16)] * (len(plain) + 1)
        + [pltpu.VMEM((width, height), BF16), pltpu.SemaphoreType.DMA((len(plain) + 1,))],
        compiler_params=pltpu.CompilerParams(vmem_limit_bytes=58 << 20),
    )(*plain, turned)
    return out[:NY], out[NY:]


def unpack(own, other):
    count = own[0].shape[1]
    rows, cols = own[0].shape[2:]
    blocks = (NZ, NY, NC, rows, cols)
    height = NZ * NY * NC * rows

    def kernel(*refs):
        ins, outs, held, across, sems = (
            refs[: 2 * NY],
            refs[2 * NY : 2 * NY + count],
            refs[2 * NY + count : -2],
            refs[-2],
            refs[-1],
        )
        y, core = place()
        copies = [
            pltpu.make_async_copy(across if i == count - 1 else held[i], outs[i], sems.at[i])
            for i in range(count)
        ]
        for i in (count - 1, *range(count - 1)):
            for d in range(NY):
                at = lax.rem(y + NY - d, NY)
                held[i][:, at, core] = ins[d][:, i]
                held[i][:, at, 1 - core] = ins[NY + d][:, i]
            if i == count - 1:
                across[...] = held[i][...].reshape(height, cols).T
            copies[i].start()
        for copy in copies:
            copy.wait()

    return pl.pallas_call(
        kernel,
        out_shape=[jax.ShapeDtypeStruct(blocks, BF16)] * (count - 1)
        + [jax.ShapeDtypeStruct((cols, height), BF16)],
        in_specs=[VMEM] * (2 * NY),
        out_specs=[HBM] * count,
        scratch_shapes=[pltpu.VMEM(blocks, BF16)] * count
        + [pltpu.VMEM((cols, height), BF16), pltpu.SemaphoreType.DMA((count,))],
        compiler_params=pltpu.CompilerParams(vmem_limit_bytes=12 << 20),
    )(*own, *other)


def butterfly(both, *steps):
    for fz, fy, fc in steps:
        moves = [(rid(z, y, c), rid(z ^ fz, y ^ fy, c ^ fc)) for z, y, c in PLACES]
        both = both + lax.ppermute(both, "replica", moves)
    return both


def gain_start(slope, param, state, me):
    width = slope.shape[-1]
    own = lax.dynamic_update_slice(
        jnp.zeros((2, width), F32), jnp.stack([param, state]), (0, me * param.shape[0])
    )
    return jnp.concatenate([slope.astype(F32).reshape(1, width), own])


def gain_end(both, me, count):
    mean = both[0] * (NZ * NY * NC) ** -0.5
    new = hold_rate * both[2] + (1.0 - hold_rate) * mean * mean
    nxt = both[1] - learn_rate * mean * lax.rsqrt(new + 1e-06)
    take = lambda v: lax.dynamic_slice(v, (me * count,), (count,))
    return nxt.astype(BF16), take(nxt), take(new)


def local(sq, sk, sv, sm, sn, pq, pk, pv, pm, pn, tq, tk, tv, tm, tn):
    me = lax.axis_index("replica")
    rows, cols = pq.shape
    slopes = [s.reshape(NZ, NY, NC, rows, cols) for s in (sq[0], sk[0], sv[0])]
    gain = gain_start(sn, pn, tn, me)

    sent, kept = pack(slopes, sm[0])
    part = [None] * NY
    for d in (1, 3, 2, 0):
        part[d] = kept[d].astype(F32) + from_core(sent[d]).astype(F32)
    came = [along_y((part[d] * 2048.0).astype(F16), d) for d in (1, 3, 2)]
    came, gain = tied(came, butterfly(gain, (3, 0, 0), (0, 1, 0)))
    came = [v.astype(F32) for v in came]
    part = part[0] + ((came[0] + came[1]) + came[2]) * 2048.0**-1
    part = across_z(part)
    part, gain = tied(part, butterfly(gain, (0, 2, 0), (1, 0, 0)))
    mean = jnp.sum(part, axis=0) * (NZ * NY * NC) ** -0.5

    param = jnp.stack([pq, pk, pv, pm.T])
    state = jnp.stack([tq, tk, tv, tm.T])
    sizes = jnp.concatenate([jnp.sum(param * param, axis=2), jnp.sum(mean * mean, axis=2)])
    sizes = over_model(sizes)
    mean = mean * (jnp.sqrt(sizes[:4]) * lax.rsqrt(sizes[4:] + 1e-06))[:, :, None]
    new = hold_rate * state + (1.0 - hold_rate) * mean * mean
    nxt = param - learn_rate * mean * lax.rsqrt(new + 1e-06)

    half = nxt.astype(BF16)
    half = across_z(jnp.broadcast_to(half, (NZ, *half.shape)))
    half, gain = tied(half, butterfly(gain, (0, 0, 1)))
    half = half.reshape(NZ, 4, rows, cols)
    own = [half] + [along_y(half, d) for d in range(1, NY)]
    own[3], gain = tied(own[3], butterfly(gain, (7, 0, 0)))
    other = [from_core(v) for v in own]
    half_norm, next_norm, new_norm = gain_end(gain, me, pn.shape[0])
    *plain, turned = unpack(own, other)
    plain = [w.reshape(-1, cols) for w in plain]
    return (
        *plain,
        turned,
        half_norm,
        nxt[0],
        nxt[1],
        nxt[2],
        nxt[3].T,
        next_norm,
        new[0],
        new[1],
        new[2],
        new[3].T,
        new_norm,
    )


def solution(mesh):
    matrix = P("replica", "model")
    turned = P("model", "replica")
    vector = P("replica")
    slope = P("replica", None, "model")
    mine = (matrix, matrix, matrix, turned, vector)
    return jax.shard_map(
        local,
        mesh=mesh,
        in_specs=(slope, slope, slope, P("replica", "model", None), P("replica", None), *mine, *mine),
        out_specs=(P(None, "model"), P(None, "model"), P(None, "model"), P("model", None), P(), *mine, *mine),
        check_vma=False,
    )
```

```python
import jax
import jax.numpy as jnp
from jax import lax
from jax.experimental import pallas as pl
from jax.experimental.pallas import tpu as pltpu
from jax.sharding import PartitionSpec as P

learn_rate = 0.025
hold_rate = 0.7

NZ, NY, NC, NX = 8, 4, 2, 4
F32, BF16, F16 = jnp.float32, jnp.bfloat16, jnp.float16
HBM = pl.BlockSpec(memory_space=pltpu.MemorySpace.HBM)
VMEM = pl.BlockSpec(memory_space=pltpu.MemorySpace.VMEM)


def rid(z, y, c):
    return (z * NY + y) * NC + c


PLACES = [(z, y, c) for z in range(NZ) for y in range(NY) for c in range(NC)]
Z_GROUPS = [[rid(z, y, c) for z in range(NZ)] for y in range(NY) for c in range(NC)]


def along_y(value, d):
    moves = [(rid(z, y, c), rid(z, (y + d) % NY, c)) for z, y, c in PLACES]
    return lax.ppermute(value, "replica", moves)


def from_core(value):
    moves = [(rid(z, y, c), rid(z, y, 1 - c)) for z, y, c in PLACES]
    return lax.ppermute(value, "replica", moves)


def across_z(value):
    return lax.all_to_all(value, "replica", 0, 0, tiled=True, axis_index_groups=Z_GROUPS)


def over_model(value):
    for flip in (1, 3):
        value = value + lax.ppermute(value, "model", [(i, i ^ flip) for i in range(NX)])
    return value


def tied(*values):
    return lax.optimization_barrier(values)


def place():
    me = lax.axis_index("replica")
    return lax.rem(lax.div(me, NC), NY), lax.rem(me, NC)


def pack(plain, turned):
    blocks = plain[0].shape
    width, height = turned.shape
    shape = (NZ, len(plain) + 1, *blocks[3:])

    def kernel(*refs):
        count = len(plain) + 1
        ins, outs, held, across, sems = (
            refs[:count],
            refs[count : -count - 2],
            refs[-count - 2 : -2],
            refs[-2],
            refs[-1],
        )
        copies = [
            pltpu.make_async_copy(ins[i], across if i == count - 1 else held[i], sems.at[i])
            for i in range(count)
        ]
        for i in (count - 1, *range(count - 1)):
            copies[i].start()
        y, core = place()
        for i in (count - 1, *range(count - 1)):
            copies[i].wait()
            if i == count - 1:
                flipped = across[...].T.reshape(blocks)
                held[i][...] = flipped
            for d in range(NY):
                at = lax.rem(y + d, NY)
                outs[d][:, i] = held[i][:, at, 1 - core]
                outs[NY + d][:, i] = held[i][:, at, core]

    out = pl.pallas_call(
        kernel,
        out_shape=[jax.ShapeDtypeStruct(shape, BF16)] * (2 * NY),
        in_specs=[HBM] * (len(plain) + 1),
        out_specs=[VMEM] * (2 * NY),
        scratch_shapes=[pltpu.VMEM(blocks, BF16)] * (len(plain) + 1)
        + [pltpu.VMEM((width, height), BF16), pltpu.SemaphoreType.DMA((len(plain) + 1,))],
        compiler_params=pltpu.CompilerParams(vmem_limit_bytes=58 << 20),
    )(*plain, turned)
    return out[:NY], out[NY:]


def unpack(own, other):
    count = own[0].shape[1]
    rows, cols = own[0].shape[2:]
    blocks = (NZ, NY, NC, rows, cols)
    height = NZ * NY * NC * rows

    def kernel(*refs):
        ins, outs, held, across, sems = (
            refs[: 2 * NY],
            refs[2 * NY : 2 * NY + count],
            refs[2 * NY + count : -2],
            refs[-2],
            refs[-1],
        )
        y, core = place()
        copies = [
            pltpu.make_async_copy(across if i == count - 1 else held[i], outs[i], sems.at[i])
            for i in range(count)
        ]
        for i in (count - 1, *range(count - 1)):
            for d in range(NY):
                at = lax.rem(y + NY - d, NY)
                held[i][:, at, core] = ins[d][:, i]
                held[i][:, at, 1 - core] = ins[NY + d][:, i]
            if i == count - 1:
                across[...] = held[i][...].reshape(height, cols).T
            copies[i].start()
        for copy in copies:
            copy.wait()

    return pl.pallas_call(
        kernel,
        out_shape=[jax.ShapeDtypeStruct(blocks, BF16)] * (count - 1)
        + [jax.ShapeDtypeStruct((cols, height), BF16)],
        in_specs=[VMEM] * (2 * NY),
        out_specs=[HBM] * count,
        scratch_shapes=[pltpu.VMEM(blocks, BF16)] * count
        + [pltpu.VMEM((cols, height), BF16), pltpu.SemaphoreType.DMA((count,))],
        compiler_params=pltpu.CompilerParams(vmem_limit_bytes=12 << 20),
    )(*own, *other)


def butterfly(both, *steps):
    for fz, fy, fc in steps:
        moves = [(rid(z, y, c), rid(z ^ fz, y ^ fy, c ^ fc)) for z, y, c in PLACES]
        both = both + lax.ppermute(both, "replica", moves)
    return both


def gain_start(slope, param, state, me):
    width = slope.shape[-1]
    own = lax.dynamic_update_slice(
        jnp.zeros((2, width), F32), jnp.stack([param, state]), (0, me * param.shape[0])
    )
    return jnp.concatenate([slope.astype(F32).reshape(1, width), own])


def gain_end(both, me, count):
    mean = both[0] * (NZ * NY * NC) ** -0.5
    new = hold_rate * both[2] + (1.0 - hold_rate) * mean * mean
    nxt = both[1] - learn_rate * mean * lax.rsqrt(new + 1e-06)
    take = lambda v: lax.dynamic_slice(v, (me * count,), (count,))
    return nxt.astype(BF16), take(nxt), take(new)


def local(sq, sk, sv, sm, sn, pq, pk, pv, pm, pn, tq, tk, tv, tm, tn):
    me = lax.axis_index("replica")
    rows, cols = pq.shape
    slopes = [s.reshape(NZ, NY, NC, rows, cols) for s in (sq[0], sk[0], sv[0])]
    gain = gain_start(sn, pn, tn, me)

    sent, kept = pack(slopes, sm[0])
    part = [None] * NY
    for d in (1, 3, 2, 0):
        part[d] = kept[d].astype(F32) + from_core(sent[d]).astype(F32)
    came = [along_y((part[d] * 2048.0).astype(F16), d) for d in (1, 3, 2)]
    came, gain = tied(came, butterfly(gain, (3, 0, 0), (0, 1, 0)))
    came = [v.astype(F32) for v in came]
    part = part[0] + ((came[0] + came[1]) + came[2]) * 2048.0**-1
    part = across_z((part * 512.0).astype(F16)).astype(F32)
    part, gain = tied(part, butterfly(gain, (0, 2, 0), (1, 0, 0)))
    mean = jnp.sum(part, axis=0) * (512.0**-1 * (NZ * NY * NC) ** -0.5)

    param = jnp.stack([pq, pk, pv, pm.T])
    state = jnp.stack([tq, tk, tv, tm.T])
    sizes = jnp.concatenate([jnp.sum(param * param, axis=2), jnp.sum(mean * mean, axis=2)])
    sizes = over_model(sizes)
    mean = mean * (jnp.sqrt(sizes[:4]) * lax.rsqrt(sizes[4:] + 1e-06))[:, :, None]
    new = hold_rate * state + (1.0 - hold_rate) * mean * mean
    nxt = param - learn_rate * mean * lax.rsqrt(new + 1e-06)

    half = nxt.astype(BF16)
    half = across_z(jnp.broadcast_to(half, (NZ, *half.shape)))
    half, gain = tied(half, butterfly(gain, (0, 0, 1)))
    half = half.reshape(NZ, 4, rows, cols)
    own = [half] + [along_y(half, d) for d in range(1, NY)]
    own[3], gain = tied(own[3], butterfly(gain, (7, 0, 0)))
    other = [from_core(v) for v in own]
    half_norm, next_norm, new_norm = gain_end(gain, me, pn.shape[0])
    *plain, turned = unpack(own, other)
    plain = [w.reshape(-1, cols) for w in plain]
    return (
        *plain,
        turned,
        half_norm,
        nxt[0],
        nxt[1],
        nxt[2],
        nxt[3].T,
        next_norm,
        new[0],
        new[1],
        new[2],
        new[3].T,
        new_norm,
    )


def solution(mesh):
    matrix = P("replica", "model")
    turned = P("model", "replica")
    vector = P("replica")
    slope = P("replica", None, "model")
    mine = (matrix, matrix, matrix, turned, vector)
    return jax.shard_map(
        local,
        mesh=mesh,
        in_specs=(slope, slope, slope, P("replica", "model", None), P("replica", None), *mine, *mine),
        out_specs=(P(None, "model"), P(None, "model"), P(None, "model"), P("model", None), P(), *mine, *mine),
        check_vma=False,
    )
```

```python
import jax
import jax.numpy as jnp
from jax import lax
from jax.experimental import pallas as pl
from jax.experimental.pallas import tpu as pltpu
from jax.sharding import PartitionSpec as P

learn_rate = 0.025
hold_rate = 0.7

NZ, NY, NC, NX = 8, 4, 2, 4
F32, BF16, F16 = jnp.float32, jnp.bfloat16, jnp.float16
HBM = pl.BlockSpec(memory_space=pltpu.MemorySpace.HBM)
VMEM = pl.BlockSpec(memory_space=pltpu.MemorySpace.VMEM)


def rid(z, y, c):
    return (z * NY + y) * NC + c


PLACES = [(z, y, c) for z in range(NZ) for y in range(NY) for c in range(NC)]
Z_GROUPS = [[rid(z, y, c) for z in range(NZ)] for y in range(NY) for c in range(NC)]


def along_y(value, d):
    moves = [(rid(z, y, c), rid(z, (y + d) % NY, c)) for z, y, c in PLACES]
    return lax.ppermute(value, "replica", moves)


def from_core(value):
    moves = [(rid(z, y, c), rid(z, y, 1 - c)) for z, y, c in PLACES]
    return lax.ppermute(value, "replica", moves)


def from_z(value, to):
    moves = [(rid(z, y, c), rid(to(z), y, c)) for z, y, c in PLACES]
    return lax.ppermute(value, "replica", moves)


def at(value, axis, index):
    return lax.dynamic_index_in_dim(value, index, axis, keepdims=False)


def across_z(value):
    return lax.all_to_all(value, "replica", 0, 0, tiled=True, axis_index_groups=Z_GROUPS)


def over_model(value):
    for flip in (1, 3):
        value = value + lax.ppermute(value, "model", [(i, i ^ flip) for i in range(NX)])
    return value


def tied(*values):
    return lax.optimization_barrier(values)


def place():
    me = lax.axis_index("replica")
    return lax.rem(lax.div(me, NC), NY), lax.rem(me, NC)


def pack(plain, turned):
    blocks = plain[0].shape
    width, height = turned.shape
    shape = (NZ, len(plain) + 1, *blocks[3:])

    def kernel(*refs):
        count = len(plain) + 1
        ins, outs, held, across, sems = (
            refs[:count],
            refs[count : -count - 2],
            refs[-count - 2 : -2],
            refs[-2],
            refs[-1],
        )
        copies = [
            pltpu.make_async_copy(ins[i], across if i == count - 1 else held[i], sems.at[i])
            for i in range(count)
        ]
        for i in (count - 1, *range(count - 1)):
            copies[i].start()
        y, core = place()
        for i in (count - 1, *range(count - 1)):
            copies[i].wait()
            if i == count - 1:
                flipped = across[...].T.reshape(blocks)
                held[i][...] = flipped
            for d in range(NY):
                at = lax.rem(y + d, NY)
                outs[d][:, i] = held[i][:, at, 1 - core]
                outs[NY + d][:, i] = held[i][:, at, core]

    out = pl.pallas_call(
        kernel,
        out_shape=[jax.ShapeDtypeStruct(shape, BF16)] * (2 * NY),
        in_specs=[HBM] * (len(plain) + 1),
        out_specs=[VMEM] * (2 * NY),
        scratch_shapes=[pltpu.VMEM(blocks, BF16)] * (len(plain) + 1)
        + [pltpu.VMEM((width, height), BF16), pltpu.SemaphoreType.DMA((len(plain) + 1,))],
        compiler_params=pltpu.CompilerParams(vmem_limit_bytes=58 << 20),
    )(*plain, turned)
    return out[:NY], out[NY:]


def unpack(own, other):
    count = own[0].shape[1]
    rows, cols = own[0].shape[2:]
    blocks = (NZ, NY, NC, rows, cols)
    height = NZ * NY * NC * rows

    def kernel(*refs):
        ins, outs, held, across, sems = (
            refs[: 2 * NY],
            refs[2 * NY : 2 * NY + count],
            refs[2 * NY + count : -2],
            refs[-2],
            refs[-1],
        )
        y, core = place()
        copies = [
            pltpu.make_async_copy(across if i == count - 1 else held[i], outs[i], sems.at[i])
            for i in range(count)
        ]
        for i in (count - 1, *range(count - 1)):
            for d in range(NY):
                at = lax.rem(y + NY - d, NY)
                held[i][:, at, core] = ins[d][:, i]
                held[i][:, at, 1 - core] = ins[NY + d][:, i]
            if i == count - 1:
                across[...] = held[i][...].reshape(height, cols).T
            copies[i].start()
        for copy in copies:
            copy.wait()

    return pl.pallas_call(
        kernel,
        out_shape=[jax.ShapeDtypeStruct(blocks, BF16)] * (count - 1)
        + [jax.ShapeDtypeStruct((cols, height), BF16)],
        in_specs=[VMEM] * (2 * NY),
        out_specs=[HBM] * count,
        scratch_shapes=[pltpu.VMEM(blocks, BF16)] * count
        + [pltpu.VMEM((cols, height), BF16), pltpu.SemaphoreType.DMA((count,))],
        compiler_params=pltpu.CompilerParams(vmem_limit_bytes=12 << 20),
    )(*own, *other)


def butterfly(both, *steps):
    for fz, fy, fc in steps:
        moves = [(rid(z, y, c), rid(z ^ fz, y ^ fy, c ^ fc)) for z, y, c in PLACES]
        both = both + lax.ppermute(both, "replica", moves)
    return both


def gain_start(slope, param, state, me):
    width = slope.shape[-1]
    own = lax.dynamic_update_slice(
        jnp.zeros((2, width), F32), jnp.stack([param, state]), (0, me * param.shape[0])
    )
    return jnp.concatenate([slope.astype(F32).reshape(1, width), own])


def gain_end(both, me, count):
    mean = both[0] * (NZ * NY * NC) ** -0.5
    new = hold_rate * both[2] + (1.0 - hold_rate) * mean * mean
    nxt = both[1] - learn_rate * mean * lax.rsqrt(new + 1e-06)
    take = lambda v: lax.dynamic_slice(v, (me * count,), (count,))
    return nxt.astype(BF16), take(nxt), take(new)


def local(sq, sk, sv, sm, sn, pq, pk, pv, pm, pn, tq, tk, tv, tm, tn):
    me = lax.axis_index("replica")
    rows, cols = pq.shape
    slopes = [s.reshape(NZ, NY, NC, rows, cols) for s in (sq[0], sk[0], sv[0])]
    gain = gain_start(sn, pn, tn, me)

    sent, kept = pack(slopes, sm[0])
    part = [None] * NY
    for d in (1, 3, 2, 0):
        part[d] = kept[d].astype(F32) + from_core(sent[d]).astype(F32)
    came = [along_y((part[d] * 2048.0).astype(F16), d) for d in (1, 3, 2)]
    came, gain = tied(came, butterfly(gain, (3, 0, 0), (0, 1, 0)))
    came = [v.astype(F32) for v in came]
    part = part[0] + ((came[0] + came[1]) + came[2]) * 2048.0**-1
    z = me // (NY * NC)
    part = part.reshape(NZ // 2, 2, *part.shape[1:])
    near = from_z((at(part, 1, 1 - z % 2) * 512.0).astype(F16), lambda z: z ^ 1)
    part = at(part, 1, z % 2) + near.astype(F32) * 512.0**-1
    far = [
        from_z(at(part, 0, (z // 2 + d) % 4), lambda z, d=d: (z + 2 * d) % NZ) for d in (1, 3, 2)
    ]
    part = (at(part, 0, z // 2) + far[2]) + (far[0] + far[1])
    part, gain = tied(part, butterfly(gain, (0, 2, 0)))
    mean = part * (NZ * NY * NC) ** -0.5

    param = jnp.stack([pq, pk, pv, pm.T])
    state = jnp.stack([tq, tk, tv, tm.T])
    sizes = jnp.concatenate([jnp.sum(param * param, axis=2), jnp.sum(mean * mean, axis=2)])
    sizes = over_model(sizes)
    mean = mean * (jnp.sqrt(sizes[:4]) * lax.rsqrt(sizes[4:] + 1e-06))[:, :, None]
    new = hold_rate * state + (1.0 - hold_rate) * mean * mean
    nxt = param - learn_rate * mean * lax.rsqrt(new + 1e-06)

    half = nxt.astype(BF16)
    half = across_z(jnp.broadcast_to(half, (NZ, *half.shape)))
    half, gain = tied(half, butterfly(gain, (0, 0, 1), (1, 0, 0)))
    half = half.reshape(NZ, 4, rows, cols)
    own = [half] + [along_y(half, d) for d in range(1, NY)]
    own[3], gain = tied(own[3], butterfly(gain, (7, 0, 0)))
    other = [from_core(v) for v in own]
    half_norm, next_norm, new_norm = gain_end(gain, me, pn.shape[0])
    *plain, turned = unpack(own, other)
    plain = [w.reshape(-1, cols) for w in plain]
    return (
        *plain,
        turned,
        half_norm,
        nxt[0],
        nxt[1],
        nxt[2],
        nxt[3].T,
        next_norm,
        new[0],
        new[1],
        new[2],
        new[3].T,
        new_norm,
    )


def solution(mesh):
    matrix = P("replica", "model")
    turned = P("model", "replica")
    vector = P("replica")
    slope = P("replica", None, "model")
    mine = (matrix, matrix, matrix, turned, vector)
    return jax.shard_map(
        local,
        mesh=mesh,
        in_specs=(slope, slope, slope, P("replica", "model", None), P("replica", None), *mine, *mine),
        out_specs=(P(None, "model"), P(None, "model"), P(None, "model"), P("model", None), P(), *mine, *mine),
        check_vma=False,
    )
```

```python
import jax
import jax.numpy as jnp
from jax import lax
from jax.experimental import pallas as pl
from jax.experimental.pallas import tpu as pltpu
from jax.sharding import PartitionSpec as P

learn_rate = 0.025
hold_rate = 0.7

NZ, NY, NC, NX = 8, 4, 2, 4
F32, BF16, F16 = jnp.float32, jnp.bfloat16, jnp.float16
HBM = pl.BlockSpec(memory_space=pltpu.MemorySpace.HBM)
VMEM = pl.BlockSpec(memory_space=pltpu.MemorySpace.VMEM)


def rid(z, y, c):
    return (z * NY + y) * NC + c


PLACES = [(z, y, c) for z in range(NZ) for y in range(NY) for c in range(NC)]
Z_GROUPS = [[rid(z, y, c) for z in range(NZ)] for y in range(NY) for c in range(NC)]


def along_y(value, d):
    moves = [(rid(z, y, c), rid(z, (y + d) % NY, c)) for z, y, c in PLACES]
    return lax.ppermute(value, "replica", moves)


def from_core(value):
    moves = [(rid(z, y, c), rid(z, y, 1 - c)) for z, y, c in PLACES]
    return lax.ppermute(value, "replica", moves)


def from_z(value, to):
    moves = [(rid(z, y, c), rid(to(z), y, c)) for z, y, c in PLACES]
    return lax.ppermute(value, "replica", moves)


def at(value, axis, index):
    return lax.dynamic_index_in_dim(value, index, axis, keepdims=False)


def across_z(value):
    return lax.all_to_all(value, "replica", 0, 0, tiled=True, axis_index_groups=Z_GROUPS)


def over_model(value):
    for flip in (1, 3):
        value = value + lax.ppermute(value, "model", [(i, i ^ flip) for i in range(NX)])
    return value


def tied(*values):
    return lax.optimization_barrier(values)


def place():
    me = lax.axis_index("replica")
    return lax.rem(lax.div(me, NC), NY), lax.rem(me, NC)


def pack(plain, turned):
    blocks = plain[0].shape
    width, height = turned.shape
    shape = (NZ, len(plain) + 1, *blocks[3:])

    def kernel(*refs):
        count = len(plain) + 1
        ins, outs, held, across, sems = (
            refs[:count],
            refs[count : -count - 2],
            refs[-count - 2 : -2],
            refs[-2],
            refs[-1],
        )
        copies = [
            pltpu.make_async_copy(ins[i], across if i == count - 1 else held[i], sems.at[i])
            for i in range(count)
        ]
        for i in (count - 1, *range(count - 1)):
            copies[i].start()
        y, core = place()
        for i in (count - 1, *range(count - 1)):
            copies[i].wait()
            if i == count - 1:
                flipped = across[...].T.reshape(blocks)
                held[i][...] = flipped
            for d in range(NY):
                at = lax.rem(y + d, NY)
                outs[d][:, i] = held[i][:, at, 1 - core]
                outs[NY + d][:, i] = held[i][:, at, core]

    out = pl.pallas_call(
        kernel,
        out_shape=[jax.ShapeDtypeStruct(shape, BF16)] * (2 * NY),
        in_specs=[HBM] * (len(plain) + 1),
        out_specs=[VMEM] * (2 * NY),
        scratch_shapes=[pltpu.VMEM(blocks, BF16)] * (len(plain) + 1)
        + [pltpu.VMEM((width, height), BF16), pltpu.SemaphoreType.DMA((len(plain) + 1,))],
        compiler_params=pltpu.CompilerParams(vmem_limit_bytes=58 << 20),
    )(*plain, turned)
    return out[:NY], out[NY:]


def unpack(own, other):
    count, rows, cols = own[0].shape[2:]
    blocks = (NZ, NY, NC, rows, cols)
    height = NZ * NY * NC * rows

    def kernel(*refs):
        ins, outs, held, across, sems = (
            refs[: 2 * NY],
            refs[2 * NY : 2 * NY + count],
            refs[2 * NY + count : -2],
            refs[-2],
            refs[-1],
        )
        y, core = place()
        pair = lax.div(lax.axis_index("replica"), 2 * NY * NC)
        copies = [
            pltpu.make_async_copy(across if i == count - 1 else held[i], outs[i], sems.at[i])
            for i in range(count)
        ]
        for i in (count - 1, *range(count - 1)):
            for d in range(NY):
                at = lax.rem(y + NY - d, NY)
                for k in range(NZ // 2):
                    z = pl.ds(2 * lax.rem(pair + NZ // 2 - k, NZ // 2), 2)
                    held[i][z, at, core] = ins[d][k, :, i]
                    held[i][z, at, 1 - core] = ins[NY + d][k, :, i]
            if i == count - 1:
                across[...] = held[i][...].reshape(height, cols).T
            copies[i].start()
        for copy in copies:
            copy.wait()

    return pl.pallas_call(
        kernel,
        out_shape=[jax.ShapeDtypeStruct(blocks, BF16)] * (count - 1)
        + [jax.ShapeDtypeStruct((cols, height), BF16)],
        in_specs=[VMEM] * (2 * NY),
        out_specs=[HBM] * count,
        scratch_shapes=[pltpu.VMEM(blocks, BF16)] * count
        + [pltpu.VMEM((cols, height), BF16), pltpu.SemaphoreType.DMA((count,))],
        compiler_params=pltpu.CompilerParams(vmem_limit_bytes=12 << 20),
    )(*own, *other)


def butterfly(both, *steps):
    for fz, fy, fc in steps:
        moves = [(rid(z, y, c), rid(z ^ fz, y ^ fy, c ^ fc)) for z, y, c in PLACES]
        both = both + lax.ppermute(both, "replica", moves)
    return both


def gain_start(slope, param, state, me):
    width = slope.shape[-1]
    own = lax.dynamic_update_slice(
        jnp.zeros((2, width), F32), jnp.stack([param, state]), (0, me * param.shape[0])
    )
    return jnp.concatenate([slope.astype(F32).reshape(1, width), own])


def gain_end(both, me, count):
    mean = both[0] * (NZ * NY * NC) ** -0.5
    new = hold_rate * both[2] + (1.0 - hold_rate) * mean * mean
    nxt = both[1] - learn_rate * mean * lax.rsqrt(new + 1e-06)
    take = lambda v: lax.dynamic_slice(v, (me * count,), (count,))
    return nxt.astype(BF16), take(nxt), take(new)


def local(sq, sk, sv, sm, sn, pq, pk, pv, pm, pn, tq, tk, tv, tm, tn):
    me = lax.axis_index("replica")
    rows, cols = pq.shape
    slopes = [s.reshape(NZ, NY, NC, rows, cols) for s in (sq[0], sk[0], sv[0])]
    gain = gain_start(sn, pn, tn, me)

    sent, kept = pack(slopes, sm[0])
    part = [None] * NY
    for d in (1, 3, 2, 0):
        part[d] = kept[d].astype(F32) + from_core(sent[d]).astype(F32)
    came = [along_y((part[d] * 2048.0).astype(F16), d) for d in (1, 3, 2)]
    came, gain = tied(came, butterfly(gain, (3, 0, 0), (0, 1, 0)))
    came = [v.astype(F32) for v in came]
    part = part[0] + ((came[0] + came[1]) + came[2]) * 2048.0**-1
    z = me // (NY * NC)
    part = part.reshape(NZ // 2, 2, *part.shape[1:])
    near = from_z((at(part, 1, 1 - z % 2) * 512.0).astype(F16), lambda z: z ^ 1)
    near, gain = tied(near, butterfly(gain, (0, 0, 1)))
    part = at(part, 1, z % 2) + near.astype(F32) * 512.0**-1
    far = [
        from_z(at(part, 0, (z // 2 + d) % 4), lambda z, d=d: (z + 2 * d) % NZ) for d in (1, 3, 2)
    ]
    part = (at(part, 0, z // 2) + far[2]) + (far[0] + far[1])
    part, gain = tied(part, butterfly(gain, (0, 2, 0)))
    mean = part * (NZ * NY * NC) ** -0.5

    param = jnp.stack([pq, pk, pv, pm.T])
    state = jnp.stack([tq, tk, tv, tm.T])
    sizes = jnp.concatenate([jnp.sum(param * param, axis=2), jnp.sum(mean * mean, axis=2)])
    sizes = over_model(sizes)
    mean = mean * (jnp.sqrt(sizes[:4]) * lax.rsqrt(sizes[4:] + 1e-06))[:, :, None]
    new = hold_rate * state + (1.0 - hold_rate) * mean * mean
    nxt = param - learn_rate * mean * lax.rsqrt(new + 1e-06)

    half = nxt.astype(BF16)
    mate = from_z(half, lambda z: z ^ 1)
    even = z % 2 == 0
    pair = jnp.stack([jnp.where(even, half, mate), jnp.where(even, mate, half)])
    half = jnp.stack(
        [pair] + [from_z(pair, lambda z, d=d: (z + 2 * d) % NZ) for d in range(1, NZ // 2)]
    )
    own = [half] + [along_y(half, d) for d in range(1, NY)]
    own[3], gain = tied(own[3], butterfly(gain, (7, 0, 0), (1, 0, 0)))
    other = [from_core(v) for v in own]
    half_norm, next_norm, new_norm = gain_end(gain, me, pn.shape[0])
    *plain, turned = unpack(own, other)
    plain = [w.reshape(-1, cols) for w in plain]
    return (
        *plain,
        turned,
        half_norm,
        nxt[0],
        nxt[1],
        nxt[2],
        nxt[3].T,
        next_norm,
        new[0],
        new[1],
        new[2],
        new[3].T,
        new_norm,
    )


def solution(mesh):
    matrix = P("replica", "model")
    turned = P("model", "replica")
    vector = P("replica")
    slope = P("replica", None, "model")
    mine = (matrix, matrix, matrix, turned, vector)
    return jax.shard_map(
        local,
        mesh=mesh,
        in_specs=(slope, slope, slope, P("replica", "model", None), P("replica", None), *mine, *mine),
        out_specs=(P(None, "model"), P(None, "model"), P(None, "model"), P("model", None), P(), *mine, *mine),
        check_vma=False,
    )
```
